32 devices in a mesh: blk: 4 (over z), team: 4 (over y, core), heads: 2 (over x).
Axes of the slice: x: 2, y: 2, z: 4, core: 2. Of those that a mesh axis runs over, the one named last changes fastest.
Arguments:
- queries: bfloat16 [512, 1024], P('blk', ('team', 'heads')), may hold values from -16 to 16
- keys: bfloat16 [512, 256], P(('blk', 'team'), 'heads'), may hold values from -16 to 16
- values: bfloat16 [512, 256], P(('blk', 'team'), 'heads'), may hold values from -6 to 6
- out_grads: bfloat16 [512, 1024], P('blk', ('team', 'heads')), may hold values from -6 to 6
- positions: int32 [512], P('blk'), may hold values from 0 to 511, as said below
Outputs:
- query_grad: bfloat16 [512, 1024], P('blk', ('team', 'heads'))
- key_grad: bfloat16 [512, 256], P(('blk', 'team'), 'heads')
- value_grad: bfloat16 [512, 256], P(('blk', 'team'), 'heads')
The draws below stay inside these ranges and needn't reach their ends.
Inputs may be any that keep to these rules, and one draw needn't show every extreme that they name: positions hold every number of 0 to 511 once; every aligned run of 32 rows holds 32 consecutive rising positions.
All inputs are finite; a program needn't handle non-finite values.
Results may differ from the reference program's by a relative error of at most 0.0069.
Values may be sent and summed in bfloat16 or wider, within the bound.
A program may use at most 64 MiB of HBM per device.

```python
import math
import jax
import jax.numpy as jnp
from jax import lax

HD = 128
PIECE = 32
KV_HEADS = 2
QUERY_HEADS = 8
TOKENS = 512


def draw_queries(key, part):
    base_draw = jnp.clip(jax.random.normal(jax.random.fold_in(key, 21), (TOKENS, QUERY_HEADS * HD), jnp.float32), -6.0, 6.0)
    return base_draw.astype(jnp.bfloat16)


def draw_keys(key, part):
    base_draw = jnp.clip(jax.random.normal(jax.random.fold_in(key, 22), (TOKENS, KV_HEADS * HD), jnp.float32), -6.0, 6.0)
    return base_draw.astype(jnp.bfloat16)


def draw_positions(key, part):
    piece_order = jax.random.permutation(jax.random.fold_in(key, 11), TOKENS // PIECE)
    placed = piece_order[:, None] * PIECE + jnp.arange(PIECE)[None, :]
    return placed.reshape(-1).astype(jnp.int32)


def block_scale(rng, extent, cuts, smallest, top_value):
    gain, own = 1.0, jax.random.fold_in(rng, 6)
    for axis_at, shards_of in cuts:
        draws = jnp.exp(jax.random.uniform(jax.random.fold_in(own, axis_at), (shards_of,), jnp.float32, smallest / len(cuts), top_value / len(cuts)))
        gain = gain * jnp.repeat(draws, extent[axis_at] // shards_of).reshape([-1 if axis == axis_at else 1 for axis in range(len(extent))])
    return gain


def bell_draw(rng, extent, spread, bound, split=(), kind=jnp.bfloat16):
    drawn = spread * jax.random.normal(rng, extent, jnp.float32)
    if split:
        drawn = drawn * block_scale(rng, extent, split, -0.22, 0.18)
    return jnp.clip(drawn, -bound, bound).astype(kind)


def setup_inputs(seed: int = 0) -> dict:
    seeds = jax.random.split(jax.random.key(seed), 6)
    return {
        "queries": draw_queries(jax.random.fold_in(seeds[5], 71), 0),
        "keys": draw_keys(jax.random.fold_in(seeds[5], 71), 0),
        "values": bell_draw(seeds[2], (TOKENS, KV_HEADS * HD), 1.0, 6.0, ((0, 16), (1, 2))),
        "out_grads": bell_draw(seeds[3], (TOKENS, QUERY_HEADS * HD), 1.0, 6.0, ((0, 4), (1, 8))),
        "positions": draw_positions(jax.random.fold_in(seeds[5], 71), 0),
    }


masked_score = -1e+30

def block_scores(query_block, grad_block, place_block, keys, values, key_places):
    head_dim = keys.shape[1]
    scale = 1.0 / math.sqrt(head_dim)
    row_count = query_block.shape[0]
    query_flat = query_block.reshape(-1, head_dim)
    grad_flat = grad_block.reshape(-1, head_dim)
    scores = jnp.dot(query_flat, keys.T, preferred_element_type=jnp.float32) * scale
    scores = scores.reshape(row_count, -1, keys.shape[0])
    visible = place_block[:, None, None] >= key_places[None, None, :]
    scores = jnp.where(visible, scores, masked_score)
    products = jnp.dot(grad_flat, values.T, preferred_element_type=jnp.float32).reshape(scores.shape)
    return (scores, products, visible)

def one_group(queries, keys, values, out_grads, places):
    head_dim = keys.shape[1]
    total = queries.shape[0]
    scale = 1.0 / math.sqrt(head_dim)
    block_rows = math.gcd(total, 128)
    blocks = total // block_rows
    query_blocks = queries.reshape(blocks, block_rows, -1, head_dim)
    grad_blocks = out_grads.reshape(blocks, block_rows, -1, head_dim)
    place_blocks = places.reshape(blocks, block_rows)

    def statistics(inputs):
        query_block, grad_block, place_block = inputs
        scores, products, visible = block_scores(query_block, grad_block, place_block, keys, values, places)
        maxima = lax.optimization_barrier(jnp.max(scores, axis=-1))
        weights = jnp.where(visible, jnp.exp(scores - maxima[..., None]), 0.0)
        totals = lax.optimization_barrier(jnp.sum(weights, axis=-1))
        traces = lax.optimization_barrier(jnp.sum(weights * products, axis=-1))
        return (maxima + jnp.log(totals), traces / totals)
    lse_all, delta_all = lax.map(statistics, (query_blocks, grad_blocks, place_blocks))

    def backward(sums_state, inputs):
        key_sum, value_sum = sums_state
        query_block, grad_block, place_block, lse_block, delta_block = inputs
        scores, products, visible = block_scores(query_block, grad_block, place_block, keys, values, places)
        weights = jnp.where(visible, jnp.exp(scores - lse_block[..., None]), 0.0)
        rounded = weights.astype(jnp.bfloat16).reshape(-1, total)
        slopes = (weights * (products - delta_block[..., None])).astype(jnp.bfloat16).reshape(-1, total)
        value_sum = value_sum + jnp.dot(rounded.T, grad_block.reshape(-1, head_dim), preferred_element_type=jnp.float32)
        key_sum = key_sum + jnp.dot(slopes.T, query_block.reshape(-1, head_dim), preferred_element_type=jnp.float32) * scale
        query_part = jnp.dot(slopes, keys, preferred_element_type=jnp.float32) * scale
        return ((key_sum, value_sum), query_part.reshape(query_block.shape).astype(jnp.bfloat16))
    zeros = jnp.zeros((total, head_dim), jnp.float32)
    (key_sum, value_sum), query_parts = lax.scan(backward, (zeros, zeros), (query_blocks, grad_blocks, place_blocks, lse_all, delta_all))
    return (query_parts.reshape(total, -1, head_dim), key_sum.astype(jnp.bfloat16), value_sum.astype(jnp.bfloat16))

def reference(queries, keys, values, out_grads, positions):
    total = queries.shape[0]
    head_dim = HD
    group_count = KV_HEADS
    places = positions.astype(jnp.float32)
    query_four = queries.reshape(total, -1, group_count, head_dim)
    grad_four = out_grads.reshape(total, -1, group_count, head_dim)
    query_list = []
    key_list = []
    value_list = []
    for group in range(group_count):
        keys_here = keys[:, group * head_dim:(group + 1) * head_dim]
        values_here = values[:, group * head_dim:(group + 1) * head_dim]
        query_part, key_part, value_part = one_group(query_four[:, :, group, :], keys_here, values_here, grad_four[:, :, group, :], places)
        query_list.append(query_part)
        key_list.append(key_part)
        value_list.append(value_part)
    query_grad = jnp.stack(query_list, 2).reshape(queries.shape)
    return (query_grad, jnp.concatenate(key_list, 1), jnp.concatenate(value_list, 1))
```

```python
import functools
import math

import jax
import jax.numpy as jnp
from jax import lax
from jax.experimental import pallas as pl
from jax.experimental.pallas import tpu as pltpu
from jax.sharding import PartitionSpec as P

masked_score = -1e30
MESH = pl.DeviceIdType.MESH


def contract_last(left, right):
    return lax.dot_general(
        left, right, (((1,), (1,)), ((), ())), preferred_element_type=jnp.float32
    )


def contract_first(left, right):
    return lax.dot_general(
        left, right, (((0,), (0,)), ((), ())), preferred_element_type=jnp.float32
    )


def each(count, body):
    if count <= 16:
        for index in range(count):
            body(index)
    else:

        def step(index, carry):
            body(index)
            return carry

        lax.fori_loop(0, count, step, 0)


def join_rows(pieces):
    count, rows, width = pieces.shape
    if rows % 16:
        return pieces.astype(jnp.float32).reshape(count * rows, width).astype(pieces.dtype)
    return pieces.reshape(count * rows, width)


def kernel(
    blocks,
    team,
    q_hbm,
    k_hbm,
    v_hbm,
    g_hbm,
    p_hbm,
    qg_hbm,
    kg_hbm,
    vg_hbm,
    q_ref,
    g_ref,
    p_ref,
    kv,
    places,
    scores,
    products,
    parts,
    landed,
    qg_ref,
    kg_ref,
    vg_ref,
    load_sem,
    kv_send,
    kv_recv,
    place_send,
    place_recv,
    part_send,
    part_recv,
    store_sem,
):
    n = blocks * team
    my_blk, my_team = lax.axis_index("blk"), lax.axis_index("team")
    me = my_blk * team + my_team
    rows, head_dim = q_ref.shape
    piece = k_hbm.shape[0]
    scale = 1.0 / math.sqrt(head_dim)

    def peer_of(index):
        step = index + 1
        blk_now = lax.rem(my_blk + lax.div(jnp.int32(step), jnp.int32(team)), blocks)
        team_now = lax.rem(my_team + lax.rem(jnp.int32(step), jnp.int32(team)), team)
        return blk_now, team_now

    loads = [
        pltpu.make_async_copy(p_hbm, p_ref, load_sem.at[0]),
        pltpu.make_async_copy(k_hbm, kv.at[me, 0], load_sem.at[1]),
        pltpu.make_async_copy(v_hbm, kv.at[me, 1], load_sem.at[2]),
        pltpu.make_async_copy(q_hbm, q_ref, load_sem.at[3]),
        pltpu.make_async_copy(g_hbm, g_ref, load_sem.at[4]),
    ]
    for load in loads:
        load.start()

    barrier = pltpu.get_barrier_semaphore()

    def greet(index):
        blk_now, team_now = peer_of(index)
        pl.semaphore_signal(
            barrier,
            inc=1,
            device_id={"blk": blk_now, "team": team_now},
            device_id_type=MESH,
        )

    each(n - 1, greet)
    loads[0].wait()
    place_row = p_ref[...].astype(jnp.float32)
    places[my_blk] = place_row
    loads[1].wait()
    loads[2].wait()
    pl.semaphore_wait(barrier, n - 1)

    def send_piece(index):
        blk_now, team_now = peer_of(n - 2 - index)
        pltpu.make_async_remote_copy(
            src_ref=kv.at[me],
            dst_ref=kv.at[me],
            send_sem=kv_send,
            recv_sem=kv_recv.at[my_blk],
            device_id={"blk": blk_now, "team": team_now},
            device_id_type=MESH,
        ).start()

    def send_places(index):
        pltpu.make_async_remote_copy(
            src_ref=places.at[my_blk],
            dst_ref=places.at[my_blk],
            send_sem=place_send,
            recv_sem=place_recv,
            device_id={"blk": lax.rem(my_blk + index + 1, blocks)},
            device_id_type=MESH,
        ).start()

    each(blocks - 1, send_places)
    each(n - 1, send_piece)
    loads[3].wait()
    loads[4].wait()
    queries = q_ref[...]
    grads = g_ref[...]

    def wait_bytes(ref, sem):
        pltpu.make_async_copy(ref, ref, sem).wait()

    def block_at(distance):
        return lax.rem(my_blk + distance, blocks)

    def block_keys(blk_now, which):
        return join_rows(kv[pl.ds(blk_now * team, team), which])

    def score_block(distance):
        blk_now = block_at(distance)
        scores[blk_now] = contract_last(block_keys(blk_now, 0), queries) * scale
        products[blk_now] = contract_last(block_keys(blk_now, 1), grads)

    wait_bytes(kv.at[pl.ds(0, team - 1)], kv_recv.at[my_blk])
    score_block(0)

    def far_block(index):
        wait_bytes(kv.at[pl.ds(0, team)], kv_recv.at[block_at(index + 1)])
        score_block(index + 1)

    each(blocks - 1, far_block)
    wait_bytes(places.at[pl.ds(0, blocks - 1)], place_recv)

    def top_of(blk_now, top):
        columns = jnp.transpose(jnp.broadcast_to(places[blk_now], (rows, rows)))
        masked = jnp.where(place_row >= columns, scores[blk_now], masked_score)
        scores[blk_now] = masked
        return jnp.maximum(top, jnp.max(masked, axis=0, keepdims=True))

    def fold(body, init):
        if blocks <= 16:
            for index in range(blocks):
                init = body(index, init)
            return init
        return lax.fori_loop(0, blocks, body, init)

    top = fold(top_of, jnp.full((1, rows), masked_score, jnp.float32))

    def sums_of(blk_now, state):
        total, trace = state
        weights = jnp.exp(scores[blk_now] - top)
        scores[blk_now] = weights
        total = total + jnp.sum(weights, axis=0, keepdims=True)
        trace = trace + jnp.sum(weights * products[blk_now], axis=0, keepdims=True)
        return total, trace

    nought = jnp.zeros((1, rows), jnp.float32)
    total, trace = fold(sums_of, (nought, nought))
    inverse = 1.0 / total
    delta = trace * inverse

    def grad_block(index, query_sum):
        blk_now = block_at(index + 1)
        weights = scores[blk_now] * inverse
        rounded = weights.astype(jnp.bfloat16)
        slopes = (weights * (products[blk_now] - delta)).astype(jnp.bfloat16)
        key_part = jnp.dot(slopes, queries, preferred_element_type=jnp.float32) * scale
        value_part = jnp.dot(rounded, grads, preferred_element_type=jnp.float32)
        group = pl.ds(blk_now * team, team)
        parts[group, 0] = key_part.reshape(team, piece, head_dim).astype(jnp.bfloat16)
        parts[group, 1] = value_part.reshape(team, piece, head_dim).astype(jnp.bfloat16)

        def send_part(team_now):
            pltpu.make_async_remote_copy(
                src_ref=parts.at[blk_now * team + team_now],
                dst_ref=landed.at[me],
                send_sem=part_send,
                recv_sem=part_recv,
                device_id={"blk": blk_now, "team": team_now},
                device_id_type=MESH,
            ).start()

        def send_home(step):
            send_part(lax.rem(my_team + step + 1, team))

        if isinstance(index, int) and index == blocks - 1:
            each(team - 1, send_home)
        else:
            each(team, send_part)
        return query_sum + contract_first(slopes, block_keys(blk_now, 0))

    query_sum = jnp.zeros((rows, head_dim), jnp.float32)
    if blocks <= 16:
        for index in range(blocks):
            query_sum = grad_block(index, query_sum)
    else:
        query_sum = lax.fori_loop(0, blocks - 1, grad_block, query_sum)
        query_sum = grad_block(blocks - 1, query_sum)

    qg_ref[...] = (query_sum * scale).astype(jnp.bfloat16)
    store_query = pltpu.make_async_copy(qg_ref, qg_hbm, store_sem.at[0])
    store_query.start()
    landed[me] = parts[me]
    wait_bytes(kv.at[pl.ds(0, n - 1)], kv_send)
    wait_bytes(places.at[pl.ds(0, blocks - 1)], place_send)
    wait_bytes(landed.at[pl.ds(0, n - 1)], part_recv)
    sums = jnp.sum(landed[...].astype(jnp.float32), axis=0)
    kg_ref[...] = sums[0].astype(jnp.bfloat16)
    vg_ref[...] = sums[1].astype(jnp.bfloat16)
    store_keys = pltpu.make_async_copy(kg_ref, kg_hbm, store_sem.at[1])
    store_values = pltpu.make_async_copy(vg_ref, vg_hbm, store_sem.at[2])
    store_keys.start()
    store_values.start()
    wait_bytes(parts.at[pl.ds(0, n - 1)], part_send)
    store_query.wait()
    store_keys.wait()
    store_values.wait()


def per_device(queries, keys, values, out_grads, positions):
    blocks, team = lax.axis_size("blk"), lax.axis_size("team")
    n = blocks * team
    rows, head_dim = queries.shape
    piece = keys.shape[0]
    any_space = pl.BlockSpec(memory_space=pl.ANY)
    return pl.pallas_call(
        functools.partial(kernel, blocks, team),
        out_shape=(
            jax.ShapeDtypeStruct(queries.shape, jnp.bfloat16),
            jax.ShapeDtypeStruct(keys.shape, jnp.bfloat16),
            jax.ShapeDtypeStruct(values.shape, jnp.bfloat16),
        ),
        in_specs=[any_space] * 5,
        out_specs=(any_space,) * 3,
        scratch_shapes=[
            pltpu.VMEM((rows, head_dim), jnp.bfloat16),
            pltpu.VMEM((rows, head_dim), jnp.bfloat16),
            pltpu.VMEM((1, rows), jnp.int32),
            pltpu.VMEM((n, 2, piece, head_dim), jnp.bfloat16),
            pltpu.VMEM((blocks, 1, rows), jnp.float32),
            pltpu.VMEM((blocks, rows, rows), jnp.float32),
            pltpu.VMEM((blocks, rows, rows), jnp.float32),
            pltpu.VMEM((n, 2, piece, head_dim), jnp.bfloat16),
            pltpu.VMEM((n, 2, piece, head_dim), jnp.bfloat16),
            pltpu.VMEM((rows, head_dim), jnp.bfloat16),
            pltpu.VMEM((piece, head_dim), jnp.bfloat16),
            pltpu.VMEM((piece, head_dim), jnp.bfloat16),
            pltpu.SemaphoreType.DMA((5,)),
            pltpu.SemaphoreType.DMA,
            pltpu.SemaphoreType.DMA((blocks,)),
            pltpu.SemaphoreType.DMA,
            pltpu.SemaphoreType.DMA,
            pltpu.SemaphoreType.DMA,
            pltpu.SemaphoreType.DMA,
            pltpu.SemaphoreType.DMA((3,)),
        ],
        compiler_params=pltpu.CompilerParams(collective_id=0, has_side_effects=True),
    )(queries, keys, values, out_grads, positions.reshape(1, rows))


def solution(mesh):
    in_specs = (
        P("blk", ("team", "heads")),
        P(("blk", "team"), "heads"),
        P(("blk", "team"), "heads"),
        P("blk", ("team", "heads")),
        P("blk"),
    )
    out_specs = (
        P("blk", ("team", "heads")),
        P(("blk", "team"), "heads"),
        P(("blk", "team"), "heads"),
    )
    return jax.shard_map(
        per_device, mesh=mesh, in_specs=in_specs, out_specs=out_specs, check_vma=False
    )
```

```python
import functools
import math

import jax
import jax.numpy as jnp
from jax import lax
from jax.experimental import pallas as pl
from jax.experimental.pallas import tpu as pltpu
from jax.sharding import PartitionSpec as P

masked_score = -1e30
MESH = pl.DeviceIdType.MESH


def contract_last(left, right):
    return lax.dot_general(
        left, right, (((1,), (1,)), ((), ())), preferred_element_type=jnp.float32
    )


def contract_first(left, right):
    return lax.dot_general(
        left, right, (((0,), (0,)), ((), ())), preferred_element_type=jnp.float32
    )


def each(count, body):
    if count <= 16:
        for index in range(count):
            body(index)
    else:

        def step(index, carry):
            body(index)
            return carry

        lax.fori_loop(0, count, step, 0)


def join_rows(pieces):
    count, rows, width = pieces.shape
    if rows % 16:
        return pieces.astype(jnp.float32).reshape(count * rows, width).astype(pieces.dtype)
    return pieces.reshape(count * rows, width)


def near_first(index, blocks):
    if index == 0:
        return 0
    return (index + 1) // 2 if index % 2 else blocks - index // 2


def kernel(
    blocks,
    team,
    q_hbm,
    k_hbm,
    v_hbm,
    g_hbm,
    p_hbm,
    qg_ref,
    kg_ref,
    vg_ref,
    q_ref,
    g_ref,
    p_ref,
    kv,
    places,
    scores,
    products,
    slopes_ref,
    parts,
    staged,
    sums_ref,
    landed,
    load_sem,
    own_send,
    own_recv,
    pass_send,
    pass_recv,
    place_send,
    place_recv,
    stage_send,
    stage_recv,
    part_send,
    part_recv,
):
    my_blk, my_team = lax.axis_index("blk"), lax.axis_index("team")
    me = my_blk * team + my_team
    rows, head_dim = q_ref.shape
    piece = k_hbm.shape[0]
    scale = 1.0 / math.sqrt(head_dim)

    def block_at(distance):
        return lax.rem(my_blk + distance, blocks)

    def mate_at(distance):
        return lax.rem(my_team + distance, team)

    def blk_peer(blk_now):
        return {"blk": blk_now, "team": my_team}

    def team_peer(team_now):
        return {"blk": my_blk, "team": team_now}

    def send(src, dst, send_sem, recv_sem, peer):
        pltpu.make_async_remote_copy(
            src_ref=src,
            dst_ref=dst,
            send_sem=send_sem,
            recv_sem=recv_sem,
            device_id=peer,
            device_id_type=MESH,
        ).start()

    def wait_bytes(ref, sem):
        pltpu.make_async_copy(ref, ref, sem).wait()

    loads = [
        pltpu.make_async_copy(p_hbm, p_ref, load_sem.at[0]),
        pltpu.make_async_copy(k_hbm, kv.at[me, 0], load_sem.at[1]),
        pltpu.make_async_copy(v_hbm, kv.at[me, 1], load_sem.at[2]),
        pltpu.make_async_copy(q_hbm, q_ref, load_sem.at[3]),
        pltpu.make_async_copy(g_hbm, g_ref, load_sem.at[4]),
    ]
    for load in loads:
        load.start()

    barrier = pltpu.get_barrier_semaphore()

    def greet(peer):
        pl.semaphore_signal(barrier, inc=1, device_id=peer, device_id_type=MESH)

    each(blocks - 1, lambda i: greet(blk_peer(block_at(i + 1))))
    each(team - 1, lambda i: greet(team_peer(mate_at(i + 1))))
    loads[0].wait()
    place_row = p_ref[...].astype(jnp.float32)
    places[my_blk] = place_row
    loads[1].wait()
    loads[2].wait()
    pl.semaphore_wait(barrier, blocks + team - 2)

    def send_far(index):
        blk_now = block_at(blocks - 1 - index)
        send(kv.at[me], kv.at[me], own_send, own_recv.at[my_blk], blk_peer(blk_now))

    def send_places(index):
        blk_now = block_at(index + 1)
        send(places.at[my_blk], places.at[my_blk], place_send, place_recv, blk_peer(blk_now))

    def pass_on(blk_now):
        slot = kv.at[blk_now * team + my_team]
        each(
            team - 1,
            lambda i: send(slot, slot, pass_send, pass_recv.at[blk_now], team_peer(mate_at(i + 1))),
        )

    each(blocks - 1, send_far)
    pass_on(my_blk)
    each(blocks - 1, send_places)

    def pass_far(distance):
        blk_now = block_at(distance)
        wait_bytes(kv.at[0], own_recv.at[blk_now])
        pass_on(blk_now)

    def block_keys(blk_now, which):
        return join_rows(kv[pl.ds(blk_now * team, team), which])

    def score_block(distance, top):
        blk_now = block_at(distance)
        wait_bytes(kv.at[pl.ds(0, team - 1)], pass_recv.at[blk_now])
        columns = jnp.transpose(jnp.broadcast_to(places[blk_now], (rows, rows)))
        found = contract_last(block_keys(blk_now, 0), queries) * scale
        masked = jnp.where(place_row >= columns, found, masked_score)
        scores[blk_now] = masked
        products[blk_now] = contract_last(block_keys(blk_now, 1), grads)
        return jnp.maximum(top, jnp.max(masked, axis=0, keepdims=True))

    def fold(body, init):
        if blocks <= 16:
            for index in range(blocks):
                init = body(index, init)
            return init
        return lax.fori_loop(0, blocks, body, init)

    loads[3].wait()
    loads[4].wait()
    queries = q_ref[...]
    grads = g_ref[...]
    top = jnp.full((1, rows), masked_score, jnp.float32)
    if blocks <= 16:
        order = [near_first(index, blocks) for index in range(blocks)]
        for distance in order[1:]:
            pass_far(distance)
        wait_bytes(places.at[pl.ds(0, blocks - 1)], place_recv)
        for distance in order:
            top = score_block(distance, top)
    else:
        order = None
        each(blocks - 1, lambda i: pass_far(i + 1))
        wait_bytes(places.at[pl.ds(0, blocks - 1)], place_recv)
        top = fold(score_block, top)

    def sums_of(blk_now, state):
        total, trace = state
        weights = jnp.exp(scores[blk_now] - top)
        scores[blk_now] = weights
        total = total + jnp.sum(weights, axis=0, keepdims=True)
        trace = trace + jnp.sum(weights * products[blk_now], axis=0, keepdims=True)
        return total, trace

    nought = jnp.zeros((1, rows), jnp.float32)
    total, trace = fold(sums_of, (nought, nought))
    inverse = 1.0 / total
    delta = trace * inverse

    def grad_block(distance):
        blk_now = block_at(distance)
        weights = scores[blk_now] * inverse
        rounded = weights.astype(jnp.bfloat16)
        slopes = (weights * (products[blk_now] - delta)).astype(jnp.bfloat16)
        slopes_ref[blk_now] = slopes
        key_part = jnp.dot(slopes, queries, preferred_element_type=jnp.float32) * scale
        value_part = jnp.dot(rounded, grads, preferred_element_type=jnp.float32)
        group = pl.ds(blk_now * team, team)
        parts[group, 0] = key_part.reshape(team, piece, head_dim).astype(jnp.bfloat16)
        parts[group, 1] = value_part.reshape(team, piece, head_dim).astype(jnp.bfloat16)

        def send_part(step):
            team_now = mate_at(step + 1)
            send(
                parts.at[blk_now * team + team_now],
                staged.at[me - my_blk * team + blk_now * team],
                stage_send,
                stage_recv.at[blk_now],
                team_peer(team_now),
            )

        each(team - 1, send_part)

    def team_sum(blk_now):
        wait_bytes(staged.at[pl.ds(0, team - 1)], stage_recv.at[blk_now])
        added = parts[blk_now * team + my_team].astype(jnp.float32)
        for step in range(team - 1):
            added = added + staged[blk_now * team + mate_at(step + 1)].astype(jnp.float32)
        return added

    def send_sum(distance):
        blk_now = block_at(distance)
        sums_ref[blk_now] = team_sum(blk_now).astype(jnp.bfloat16)
        send(sums_ref.at[blk_now], landed.at[my_blk], part_send, part_recv, blk_peer(blk_now))

    def add_query(blk_now, query_sum):
        return query_sum + contract_first(slopes_ref[blk_now], block_keys(blk_now, 0))

    if order:
        for distance in order[::-1]:
            grad_block(distance)
    else:
        each(blocks, lambda i: grad_block(i))
    query_sum = fold(add_query, jnp.zeros((rows, head_dim), jnp.float32))
    qg_ref[...] = (query_sum * scale).astype(jnp.bfloat16)
    if order:
        for distance in order[:0:-1]:
            send_sum(distance)
    else:
        each(blocks - 1, lambda i: send_sum(i + 1))
    sums = team_sum(my_blk)
    wait_bytes(kv.at[pl.ds(0, blocks - 1)], own_send)
    wait_bytes(kv.at[pl.ds(0, blocks * (team - 1))], pass_send)
    wait_bytes(places.at[pl.ds(0, blocks - 1)], place_send)
    wait_bytes(staged.at[pl.ds(0, blocks * (team - 1))], stage_send)
    wait_bytes(landed.at[pl.ds(0, blocks - 1)], part_recv)

    def add_landed(index, sums):
        return sums + landed[block_at(index + 1)].astype(jnp.float32)

    if blocks <= 16:
        for index in range(blocks - 1):
            sums = add_landed(index, sums)
    else:
        sums = lax.fori_loop(0, blocks - 1, add_landed, sums)
    kg_ref[...] = sums[0].astype(jnp.bfloat16)
    vg_ref[...] = sums[1].astype(jnp.bfloat16)
    wait_bytes(sums_ref.at[pl.ds(0, blocks - 1)], part_send)


def put_out(*refs):
    count = (len(refs) - 1) // 2
    copies = [
        pltpu.make_async_copy(refs[i], refs[count + i], refs[-1].at[i]) for i in range(count)
    ]
    for copy in copies:
        copy.start()
    for copy in copies:
        copy.wait()


def per_device(queries, keys, values, out_grads, positions):
    blocks, team = lax.axis_size("blk"), lax.axis_size("team")
    n = blocks * team
    rows, head_dim = queries.shape
    piece = keys.shape[0]
    any_space = pl.BlockSpec(memory_space=pl.ANY)
    near_space = pl.BlockSpec(memory_space=pltpu.VMEM)
    results = (queries, keys, values)
    sends = pltpu.SemaphoreType.DMA
    many = pltpu.SemaphoreType.DMA((blocks,))
    slots = pltpu.VMEM((n, 2, piece, head_dim), jnp.bfloat16)
    few = pltpu.VMEM((blocks, 2, piece, head_dim), jnp.bfloat16)
    square = pltpu.VMEM((blocks, rows, rows), jnp.float32)
    held = pl.pallas_call(
        functools.partial(kernel, blocks, team),
        out_shape=tuple(pltpu.VMEM(one.shape, jnp.bfloat16) for one in results),
        in_specs=[any_space] * 5,
        out_specs=(near_space,) * 3,
        scratch_shapes=[
            pltpu.VMEM((rows, head_dim), jnp.bfloat16),
            pltpu.VMEM((rows, head_dim), jnp.bfloat16),
            pltpu.VMEM((1, rows), jnp.int32),
            slots,
            pltpu.VMEM((blocks, 1, rows), jnp.float32),
            square,
            square,
            pltpu.VMEM((blocks, rows, rows), jnp.bfloat16),
            slots,
            slots,
            few,
            few,
            pltpu.SemaphoreType.DMA((5,)),
            sends,
            many,
            sends,
            many,
            sends,
            sends,
            sends,
            many,
            sends,
            sends,
        ],
        compiler_params=pltpu.CompilerParams(collective_id=0, has_side_effects=True),
    )(queries, keys, values, out_grads, positions.reshape(1, rows))
    return pl.pallas_call(
        put_out,
        out_shape=tuple(jax.ShapeDtypeStruct(one.shape, jnp.bfloat16) for one in results),
        in_specs=[near_space] * 3,
        out_specs=(any_space,) * 3,
        scratch_shapes=[pltpu.SemaphoreType.DMA((3,))],
    )(*(pltpu.with_memory_space_constraint(one, pltpu.VMEM) for one in held))


def solution(mesh):
    in_specs = (
        P("blk", ("team", "heads")),
        P(("blk", "team"), "heads"),
        P(("blk", "team"), "heads"),
        P("blk", ("team", "heads")),
        P("blk"),
    )
    out_specs = (
        P("blk", ("team", "heads")),
        P(("blk", "team"), "heads"),
        P(("blk", "team"), "heads"),
    )
    return jax.shard_map(
        per_device, mesh=mesh, in_specs=in_specs, out_specs=out_specs, check_vma=False
    )
```

```python
import functools
import math

import jax
import jax.numpy as jnp
from jax import lax
from jax.experimental import pallas as pl
from jax.experimental.pallas import tpu as pltpu
from jax.sharding import PartitionSpec as P

masked_score = -1e30
MESH = pl.DeviceIdType.MESH


def contract_last(left, right):
    return lax.dot_general(
        left, right, (((1,), (1,)), ((), ())), preferred_element_type=jnp.float32
    )


def contract_first(left, right):
    return lax.dot_general(
        left, right, (((0,), (0,)), ((), ())), preferred_element_type=jnp.float32
    )


def each(count, body):
    if count <= 16:
        for index in range(count):
            body(index)
    else:

        def step(index, carry):
            body(index)
            return carry

        lax.fori_loop(0, count, step, 0)


def join_rows(pieces):
    count, rows, width = pieces.shape
    if rows % 16:
        return pieces.astype(jnp.float32).reshape(count * rows, width).astype(pieces.dtype)
    return pieces.reshape(count * rows, width)


def near_first(index, blocks):
    if index == 0:
        return 0
    return (index + 1) // 2 if index % 2 else blocks - index // 2


def kernel(
    blocks,
    team,
    q_hbm,
    k_hbm,
    v_hbm,
    g_hbm,
    p_hbm,
    qg_ref,
    kg_ref,
    vg_ref,
    q_ref,
    g_ref,
    p_ref,
    kv,
    places,
    scores,
    products,
    slopes_ref,
    columns,
    tops,
    parts,
    staged,
    sums_ref,
    landed,
    load_sem,
    own_send,
    own_recv,
    pass_send,
    pass_recv,
    place_send,
    place_recv,
    stage_send,
    stage_recv,
    part_send,
    part_recv,
):
    my_blk, my_team = lax.axis_index("blk"), lax.axis_index("team")
    me = my_blk * team + my_team
    rows, head_dim = q_ref.shape
    piece = k_hbm.shape[0]
    scale = 1.0 / math.sqrt(head_dim)

    def block_at(distance):
        return lax.rem(my_blk + distance, blocks)

    def mate_at(distance):
        return lax.rem(my_team + distance, team)

    def blk_peer(blk_now):
        return {"blk": blk_now, "team": my_team}

    def team_peer(team_now):
        return {"blk": my_blk, "team": team_now}

    def send(src, dst, send_sem, recv_sem, peer):
        pltpu.make_async_remote_copy(
            src_ref=src,
            dst_ref=dst,
            send_sem=send_sem,
            recv_sem=recv_sem,
            device_id=peer,
            device_id_type=MESH,
        ).start()

    def wait_bytes(ref, sem):
        pltpu.make_async_copy(ref, ref, sem).wait()

    barrier = pltpu.get_barrier_semaphore()

    def greet(peer):
        pl.semaphore_signal(barrier, inc=1, device_id=peer, device_id_type=MESH)

    each(blocks - 1, lambda i: greet(blk_peer(block_at(blocks - 1 - i))))
    each(team - 1, lambda i: greet(team_peer(mate_at(i + 1))))
    loads = [
        pltpu.make_async_copy(p_hbm, p_ref, load_sem.at[0]),
        pltpu.make_async_copy(k_hbm, kv.at[me, 0], load_sem.at[1]),
        pltpu.make_async_copy(v_hbm, kv.at[me, 1], load_sem.at[2]),
        pltpu.make_async_copy(q_hbm, q_ref, load_sem.at[3]),
        pltpu.make_async_copy(g_hbm, g_ref, load_sem.at[4]),
    ]
    for which in (1, 2, 0, 3, 4):
        loads[which].start()

    loads[0].wait()
    place_row = p_ref[...].astype(jnp.float32)
    places[my_blk] = place_row
    loads[1].wait()
    loads[2].wait()
    pl.semaphore_wait(barrier, blocks + team - 2)

    def send_far(index):
        blk_now = block_at(blocks - 1 - index)
        send(kv.at[me], kv.at[me], own_send, own_recv.at[my_blk], blk_peer(blk_now))

    def send_places(index):
        blk_now = block_at(index + 1)
        send(places.at[my_blk], places.at[my_blk], place_send, place_recv, blk_peer(blk_now))

    def pass_on(blk_now):
        slot = kv.at[blk_now * team + my_team]
        each(
            team - 1,
            lambda i: send(slot, slot, pass_send, pass_recv.at[blk_now], team_peer(mate_at(i + 1))),
        )

    each(blocks - 1, send_far)
    pass_on(my_blk)
    each(blocks - 1, send_places)

    def pass_far(distance):
        blk_now = block_at(distance)
        wait_bytes(kv.at[0], own_recv.at[blk_now])
        pass_on(blk_now)

    def block_keys(blk_now, which):
        return join_rows(kv[pl.ds(blk_now * team, team), which])

    def make_columns(blk_now):
        columns[blk_now] = jnp.transpose(jnp.broadcast_to(places[blk_now], (rows, rows)))

    def score_block(distance, state):
        top, total, trace = state
        blk_now = block_at(distance)
        wait_bytes(kv.at[pl.ds(0, team - 1)], pass_recv.at[blk_now])
        found = contract_last(block_keys(blk_now, 0), queries) * scale
        block_products = contract_last(block_keys(blk_now, 1), grads)
        masked = jnp.where(place_row >= columns[blk_now], found, masked_score)
        updated = jnp.maximum(top, jnp.max(masked, axis=0, keepdims=True))
        weights = jnp.exp(masked - updated)
        scores[blk_now] = weights
        products[blk_now] = block_products
        tops[blk_now] = updated
        factor = jnp.exp(top - updated)
        total = total * factor + jnp.sum(weights, axis=0, keepdims=True)
        trace = trace * factor + jnp.sum(weights * block_products, axis=0, keepdims=True)
        return updated, total, trace

    def fold(body, init):
        if blocks <= 16:
            for index in range(blocks):
                init = body(index, init)
            return init
        return lax.fori_loop(0, blocks, body, init)

    loads[3].wait()
    loads[4].wait()
    queries = q_ref[...]
    grads = g_ref[...]
    nought = jnp.zeros((1, rows), jnp.float32)
    state = (jnp.full((1, rows), masked_score, jnp.float32), nought, nought)
    if blocks <= 16:
        order = [near_first(index, blocks) for index in range(blocks)]
        for distance in order[1:]:
            pass_far(distance)
        wait_bytes(places.at[pl.ds(0, blocks - 1)], place_recv)
        each(blocks, make_columns)
        for distance in order:
            state = score_block(distance, state)
    else:
        order = None
        each(blocks - 1, lambda i: pass_far(i + 1))
        wait_bytes(places.at[pl.ds(0, blocks - 1)], place_recv)
        each(blocks, make_columns)
        state = fold(score_block, state)
    top, total, trace = state
    inverse = 1.0 / total
    delta = trace * inverse

    def grad_block(distance):
        blk_now = block_at(distance)
        weights = scores[blk_now] * (inverse * jnp.exp(tops[blk_now] - top))
        rounded = weights.astype(jnp.bfloat16)
        slopes = (weights * (products[blk_now] - delta)).astype(jnp.bfloat16)
        slopes_ref[blk_now] = slopes
        key_part = jnp.dot(slopes, queries, preferred_element_type=jnp.float32) * scale
        value_part = jnp.dot(rounded, grads, preferred_element_type=jnp.float32)
        group = pl.ds(blk_now * team, team)
        parts[group, 0] = key_part.reshape(team, piece, head_dim).astype(jnp.bfloat16)
        parts[group, 1] = value_part.reshape(team, piece, head_dim).astype(jnp.bfloat16)

        def send_part(step):
            team_now = mate_at(step + 1)
            send(
                parts.at[blk_now * team + team_now],
                staged.at[me - my_blk * team + blk_now * team],
                stage_send,
                stage_recv.at[blk_now],
                team_peer(team_now),
            )

        each(team - 1, send_part)

    def team_sum(blk_now):
        wait_bytes(staged.at[pl.ds(0, team - 1)], stage_recv.at[blk_now])
        added = parts[blk_now * team + my_team].astype(jnp.float32)
        for step in range(team - 1):
            added = added + staged[blk_now * team + mate_at(step + 1)].astype(jnp.float32)
        return added

    def send_sum(distance):
        blk_now = block_at(distance)
        sums_ref[blk_now] = team_sum(blk_now).astype(jnp.bfloat16)
        send(sums_ref.at[blk_now], landed.at[my_blk], part_send, part_recv, blk_peer(blk_now))

    def add_query(blk_now, query_sum):
        return query_sum + contract_first(slopes_ref[blk_now], block_keys(blk_now, 0))

    if order:
        for distance in order[::-1]:
            grad_block(distance)
    else:
        each(blocks, lambda i: grad_block(i))
    query_sum = fold(add_query, jnp.zeros((rows, head_dim), jnp.float32))
    qg_ref[...] = (query_sum * scale).astype(jnp.bfloat16)
    if order:
        for distance in order[:0:-1]:
            send_sum(distance)
    else:
        each(blocks - 1, lambda i: send_sum(i + 1))
    sums = team_sum(my_blk)
    wait_bytes(kv.at[pl.ds(0, blocks - 1)], own_send)
    wait_bytes(kv.at[pl.ds(0, blocks * (team - 1))], pass_send)
    wait_bytes(places.at[pl.ds(0, blocks - 1)], place_send)
    wait_bytes(staged.at[pl.ds(0, blocks * (team - 1))], stage_send)
    wait_bytes(landed.at[pl.ds(0, blocks - 1)], part_recv)

    def add_landed(index, sums):
        return sums + landed[block_at(index + 1)].astype(jnp.float32)

    if blocks <= 16:
        for index in range(blocks - 1):
            sums = add_landed(index, sums)
    else:
        sums = lax.fori_loop(0, blocks - 1, add_landed, sums)
    kg_ref[...] = sums[0].astype(jnp.bfloat16)
    vg_ref[...] = sums[1].astype(jnp.bfloat16)
    wait_bytes(sums_ref.at[pl.ds(0, blocks - 1)], part_send)


def put_out(*refs):
    count = (len(refs) - 1) // 2
    copies = [
        pltpu.make_async_copy(refs[i], refs[count + i], refs[-1].at[i]) for i in range(count)
    ]
    for copy in copies:
        copy.start()
    for copy in copies:
        copy.wait()


def per_device(queries, keys, values, out_grads, positions):
    blocks, team = lax.axis_size("blk"), lax.axis_size("team")
    n = blocks * team
    rows, head_dim = queries.shape
    piece = keys.shape[0]
    any_space = pl.BlockSpec(memory_space=pl.ANY)
    near_space = pl.BlockSpec(memory_space=pltpu.VMEM)
    results = (queries, keys, values)
    sends = pltpu.SemaphoreType.DMA
    many = pltpu.SemaphoreType.DMA((blocks,))
    slots = pltpu.VMEM((n, 2, piece, head_dim), jnp.bfloat16)
    few = pltpu.VMEM((blocks, 2, piece, head_dim), jnp.bfloat16)
    square = pltpu.VMEM((blocks, rows, rows), jnp.float32)
    held = pl.pallas_call(
        functools.partial(kernel, blocks, team),
        out_shape=tuple(pltpu.VMEM(one.shape, jnp.bfloat16) for one in results),
        in_specs=[any_space] * 5,
        out_specs=(near_space,) * 3,
        scratch_shapes=[
            pltpu.VMEM((rows, head_dim), jnp.bfloat16),
            pltpu.VMEM((rows, head_dim), jnp.bfloat16),
            pltpu.VMEM((1, rows), jnp.int32),
            slots,
            pltpu.VMEM((blocks, 1, rows), jnp.float32),
            square,
            square,
            pltpu.VMEM((blocks, rows, rows), jnp.bfloat16),
            square,
            pltpu.VMEM((blocks, 1, rows), jnp.float32),
            slots,
            slots,
            few,
            few,
            pltpu.SemaphoreType.DMA((5,)),
            sends,
            many,
            sends,
            many,
            sends,
            sends,
            sends,
            many,
            sends,
            sends,
        ],
        compiler_params=pltpu.CompilerParams(collective_id=0, has_side_effects=True),
    )(queries, keys, values, out_grads, positions.reshape(1, rows))
    return pl.pallas_call(
        put_out,
        out_shape=tuple(jax.ShapeDtypeStruct(one.shape, jnp.bfloat16) for one in results),
        in_specs=[near_space] * 3,
        out_specs=(any_space,) * 3,
        scratch_shapes=[pltpu.SemaphoreType.DMA((3,))],
    )(*(pltpu.with_memory_space_constraint(one, pltpu.VMEM) for one in held))


def solution(mesh):
    in_specs = (
        P("blk", ("team", "heads")),
        P(("blk", "team"), "heads"),
        P(("blk", "team"), "heads"),
        P("blk", ("team", "heads")),
        P("blk"),
    )
    out_specs = (
        P("blk", ("team", "heads")),
        P(("blk", "team"), "heads"),
        P(("blk", "team"), "heads"),
    )
    return jax.shard_map(
        per_device, mesh=mesh, in_specs=in_specs, out_specs=out_specs, check_vma=False
    )
```
